32 devices in a mesh: box: 2 (over x), dir: 16 (over z, y, core).
Axes of the slice: x: 2, y: 2, z: 4, core: 2. Of those that a mesh axis runs over, the one named last changes fastest.
Arguments:
- leaf_patterns: bfloat16 [512, 2, 8, 1024], P(('box', 'dir')), may hold values from -6 to 6
- octant: int32 [512], P(('box', 'dir')), may hold values from 0 to 7, as said below
- interp: bfloat16 [1024, 4096], replicated, may hold values from -0.1875 to 0.1875
- shift_angle: float32 [8, 4096], replicated, may hold values from -3.140625 to 3.140625
- partners: int32 [64, 27], P('box'), may hold values from 0 to 63, as said below
- types: int32 [64, 27], P('box'), may hold values from 0 to 342, as said below
- translators: float32 [343, 2, 4096], P(None, None, 'dir'), may hold values from -1 to 1
Outputs:
- leaf_incoming: bfloat16 [512, 2, 8, 1024], P(('box', 'dir'))
The draws below stay inside these ranges and needn't reach their ends.
Inputs may be any that keep to these rules, and one draw needn't show every extreme that they name: The leaf boxes 8 p to 8 p + 7 are the children of parent box p; octant gives each child its position in the parent, each of 0 to 7 once among the 8 children. Parent boxes form a grid indexed in Morton order (bit j of the index is a bit of coordinate j % 3). The 27 partners of a box are distinct boxes within three boxes of it along every dimension, and none is the box itself or one of its 26 neighbours. types[p, k] = 49 (dx + 3) + 7 (dy + 3) + (dz + 3), where (dx, dy, dz) is the grid offset from box p to partners[p, k].
All inputs are finite; a program needn't handle non-finite values.
Results may differ from the reference program's by a relative error of at most 0.0064.
Values may be sent and summed in bfloat16 or wider, within the bound.
No kernel may reach another device: no remote copies, remote signals or barrier semaphores. Data moves between devices by JAX's collectives and lax.ppermute only.
A program may use at most 64 MiB of HBM per device.

```python
import jax
import jax.numpy as jnp
from jax import lax

NDIR_L = 1024
NDIR_P = 4096
EXC = 8
OFFSETS = 343
NB_L = 512
NB_P = 64


def geometry(key):
    levels = NB_P.bit_length() - 1
    index = jnp.arange(NB_P, dtype=jnp.int32)
    coords = [jnp.zeros((NB_P,), jnp.int32) for axis_id in range(3)]
    extent = [1, 1, 1]
    for bit in range(levels):
        axis_id = bit % 3
        coords[axis_id] = coords[axis_id] + index // 2 ** bit % 2 * 2 ** (bit // 3)
        extent[axis_id] = extent[axis_id] * 2
    offset = jnp.arange(343, dtype=jnp.int32)
    deltas = [offset // 49 - 3, offset // 7 % 7 - 3, offset % 7 - 3]
    inside = jnp.ones((NB_P, 343), dtype=bool)
    target_coords = []
    for axis_id in range(3):
        moved = coords[axis_id][:, None] + deltas[axis_id][None, :]
        inside = inside & (moved >= 0) & (moved < extent[axis_id])
        target_coords.append(jnp.clip(moved, 0, extent[axis_id] - 1))
    reach = jnp.maximum(jnp.maximum(jnp.abs(deltas[0]), jnp.abs(deltas[1])), jnp.abs(deltas[2]))
    valid = inside & (reach >= 2)[None, :]
    target = jnp.zeros((NB_P, 343), jnp.int32)
    for bit in range(levels):
        axis_id = bit % 3
        target = target + target_coords[axis_id] // 2 ** (bit // 3) % 2 * 2 ** bit
    scores = jax.random.randint(jax.random.fold_in(key, 7), (NB_P, 343), 0, 65536) * 343 + offset[None, :]
    scores = jnp.where(valid, scores, -1)
    chosen = lax.top_k(scores, 27)[1].astype(jnp.int32)
    linked = jnp.take_along_axis(target, chosen, axis=1).astype(jnp.int32)
    return (linked, chosen)


def draw_partners(key, part):
    return geometry(key)[0]


def draw_types(key, part):
    return geometry(key)[1]


def draw_octant(key, part):
    groups = NB_L // 8
    scores = jax.random.randint(jax.random.fold_in(key, 3), (groups, 8), 0, 65536) * 8 + jnp.arange(8, dtype=jnp.int32)[None, :]
    order = jnp.argsort(scores, axis=1, stable=True)
    return order.reshape(-1).astype(jnp.int32)


def level_of(key, dims, split, least, top_value):
    factor_of = 1.0
    for axis_at, parts in split:
        steps = jax.random.uniform(jax.random.fold_in(jax.random.fold_in(key, 6), axis_at), (parts,), jnp.float32, least / len(split), top_value / len(split))
        factor_of = factor_of * jnp.repeat(jnp.exp(steps), dims[axis_at] // parts).reshape((-1,) + (1,) * (len(dims) - 1 - axis_at))
    return factor_of


def scatter_about(stream_key, shape, width, limit, shards=(), kind=jnp.bfloat16):
    array = width * jax.random.normal(stream_key, shape, jnp.float32)
    if shards:
        array = array * level_of(stream_key, shape, shards, -0.22, 0.18)
    return jnp.clip(array, -limit, limit).astype(kind)


def setup_inputs(seed: int = 0) -> dict:
    key_of = jax.random.split(jax.random.key(seed), 8)
    return {
        "leaf_patterns": scatter_about(key_of[0], (NB_L, 2, EXC, NDIR_L), 1.0, 6.0, ((0, 32),)),
        "octant": draw_octant(jax.random.fold_in(key_of[7], 71), 0),
        "interp": scatter_about(key_of[2], (NDIR_L, NDIR_P), NDIR_L ** -0.5, 0.1875),
        "shift_angle": jnp.clip(jax.random.uniform(key_of[3], (8, NDIR_P), jnp.float32, -3.140625, 3.140625), -3.140625, 3.140625),
        "partners": draw_partners(jax.random.fold_in(key_of[7], 71), 0),
        "types": draw_types(jax.random.fold_in(key_of[7], 71), 0),
        "translators": scatter_about(key_of[6], (OFFSETS, 2, NDIR_P), 0.15, 1.0, ((2, 16),), jnp.float32),
    }


def reference(leaf_patterns, octant, interp, shift_angle, partners, types, translators):
    cosines = jnp.cos(shift_angle)
    sines = jnp.sin(shift_angle)
    boxes, pairs, excite, low = leaf_patterns.shape
    high = interp.shape[1]
    parents = boxes // 8
    block = min(64, parents)
    count = parents // block

    def lift(item):
        leaf_block, octant_block = item
        up = jnp.dot(leaf_block.reshape(-1, low), interp, preferred_element_type=jnp.float32)
        up = up.reshape(block * 8, 2, excite, high)
        cos_child = cosines[octant_block][:, None, :]
        sin_child = sines[octant_block][:, None, :]
        real = up[:, 0] * cos_child - up[:, 1] * sin_child
        imag = up[:, 0] * sin_child + up[:, 1] * cos_child
        summed = jnp.stack([real, imag], 1).reshape(block, 8, 2, excite, high).sum(axis=1)
        return summed.astype(jnp.bfloat16)

    aggregated = lax.map(lift, (leaf_patterns.reshape(count, block * 8, 2, excite, low),
                                octant.reshape(count, block * 8)))
    aggregated = aggregated.reshape(parents, 2, excite, high)

    def translate(step, total):
        source = jnp.take(aggregated, partners[:, step], axis=0).astype(jnp.float32)
        factor = jnp.take(translators, types[:, step], axis=0)
        factor_re = factor[:, 0][:, None, :]
        factor_im = factor[:, 1][:, None, :]
        real = factor_re * source[:, 0] - factor_im * source[:, 1]
        imag = factor_re * source[:, 1] + factor_im * source[:, 0]
        return total + jnp.stack([real, imag], 1)

    zero = jnp.zeros((parents, 2, excite, high), jnp.float32)
    incoming = lax.fori_loop(0, partners.shape[1], translate, zero).astype(jnp.bfloat16)
    scale = low / high

    def descend(item):
        parent_block, octant_block = item
        spread = jnp.repeat(parent_block.astype(jnp.float32), 8, axis=0)
        cos_child = cosines[octant_block][:, None, :]
        sin_child = sines[octant_block][:, None, :]
        real = spread[:, 0] * cos_child + spread[:, 1] * sin_child
        imag = spread[:, 1] * cos_child - spread[:, 0] * sin_child
        shifted = jnp.stack([real, imag], 1).astype(jnp.bfloat16).reshape(-1, high)
        down = lax.dot_general(shifted, interp, (((1,), (1,)), ((), ())), preferred_element_type=jnp.float32)
        return (down * scale).astype(jnp.bfloat16).reshape(block * 8, 2, excite, low)

    leaf_incoming = lax.map(descend, (incoming.reshape(count, block, 2, excite, high),
                                      octant.reshape(count, block * 8)))
    return leaf_incoming.reshape(boxes, 2, excite, low)
```

```python
import functools

import jax
import jax.numpy as jnp
from jax import lax
from jax.experimental import pallas as pl
from jax.experimental.pallas import tpu as pltpu
from jax.sharding import PartitionSpec as P

LANES = 128
EXCITE = 8
PAIR = 2 * EXCITE
MIB = 1 << 20
AHEAD = 2


def sincos(x):
    turns = jnp.floor(x * 0.6366197723675814 + 0.5)
    r = x - turns * 1.5703125
    r = r - turns * 4.837512969970703e-4
    r = r - turns * 7.549789948768648e-8
    z = r * r
    s = ((-1.9515295891e-4 * z + 8.3321608736e-3) * z - 1.6666654611e-1) * z * r + r
    c = ((2.443315711809948e-5 * z - 1.388731625493765e-3) * z + 4.166664568298827e-2) * z * z
    c = c - 0.5 * z + 1.0
    quadrant = turns.astype(jnp.int32)
    odd = (quadrant & 1) == 1
    sine = jnp.where(odd, c, s)
    cosine = jnp.where(odd, s, c)
    sine = jnp.where((quadrant & 2) == 2, -sine, sine)
    cosine = jnp.where(((quadrant + 1) & 2) == 2, -cosine, cosine)
    return cosine, sine


def phases(angle, cosines, sines):
    def block(b, carry):
        lanes = pl.ds(pl.multiple_of(b * LANES, LANES), LANES)
        cosines[b], sines[b] = sincos(angle[:, lanes])
        return carry

    lax.fori_loop(0, cosines.shape[0], block, 0, unroll=4)


def chunk_of(i, tile):
    return pl.ds(pl.multiple_of(i * tile, tile), tile)


def column_copy(far, near, arrived, tile, i):
    columns = chunk_of(i, tile)
    return pltpu.make_async_copy(far.at[:, columns], near.at[:, columns], arrived.at[i])


def lift_kernel(
    place, tile, octant_far, leaf_far, interp_far, angle_far, out_far,
    octant, leaf, interp, angle, cosines, sines, up_even, up_odd, out, arrived, ready, sent,
):
    low, high = interp.shape
    count = high // tile
    boxes = leaf.shape[0] // PAIR
    angle_copy = pltpu.make_async_copy(angle_far, angle, ready.at[0])
    leaf_copy = pltpu.make_async_copy(leaf_far, leaf, ready.at[1])
    octant_copy = pltpu.make_async_copy(octant_far, octant, ready.at[2])
    angle_copy.start()
    octant_copy.start()
    leaf_copy.start()
    ahead = min(AHEAD, count)
    for i in range(ahead):
        column_copy(interp_far, interp, arrived, tile, i).start()
    angle_copy.wait()
    phases(angle, cosines, sines)
    octant_copy.wait()
    leaf_copy.wait()

    def send(i, first, last):
        for part in range(tile // LANES):
            block = place(i * (tile // LANES) + part)
            copy = pltpu.make_async_copy(out.at[block], out_far.at[block], sent.at[block])
            copy.start() if first else None
            copy.wait() if last else None

    def rise(i, up):
        column_copy(interp_far, interp, arrived, tile, i).wait()

        @pl.when(i + ahead < count)
        def _():
            column_copy(interp_far, interp, arrived, tile, i + ahead).start()

        up[...] = jnp.dot(
            leaf[...], interp[:, chunk_of(i, tile)], preferred_element_type=jnp.float32
        )

    def combine(i, up):
        for lane in range(0, tile, LANES):
            block = i * (tile // LANES) + lane // LANES
            for parent in range(boxes // 8):
                real = imag = None
                for child in range(8 * parent, 8 * parent + 8):
                    which = octant[child]
                    cos = cosines[block, pl.ds(which, 1), :]
                    sin = sines[block, pl.ds(which, 1), :]
                    row = PAIR * child
                    up_re = up[row : row + EXCITE, lane : lane + LANES]
                    up_im = up[row + EXCITE : row + PAIR, lane : lane + LANES]
                    re = up_re * cos - up_im * sin
                    im = up_re * sin + up_im * cos
                    real = re if real is None else real + re
                    imag = im if imag is None else imag + im
                both = jnp.concatenate([real, imag], 0).astype(jnp.bfloat16)
                out[place(block), PAIR * parent : PAIR * (parent + 1), :] = both

    def two(j, carry):
        @pl.when(j > 0)
        def _():
            send(2 * j - 2, True, False)

        rise(2 * j, up_even)
        combine(jnp.maximum(2 * j - 1, 0), up_odd)
        rise(2 * j + 1, up_odd)
        combine(2 * j, up_even)
        return carry

    lax.fori_loop(0, count // 2, two, 0)
    combine(count - 1, up_odd)
    for i in range(count):
        if i % 2 or i + 2 >= count:
            send(i, True, False)
    for i in range(count):
        send(i, False, True)


def lift(leaf, octant, interp, angle, place):
    rows, low = leaf.shape
    high = interp.shape[1]
    tile = 1024
    far = pl.BlockSpec(memory_space=pltpu.HBM)
    return pl.pallas_call(
        functools.partial(lift_kernel, place, tile),
        out_shape=jax.ShapeDtypeStruct((high // LANES, rows // 8, LANES), jnp.bfloat16),
        in_specs=[far, far, far, far],
        out_specs=far,
        scratch_shapes=[
            pltpu.SMEM(octant.shape, octant.dtype),
            pltpu.VMEM(leaf.shape, leaf.dtype),
            pltpu.VMEM(interp.shape, interp.dtype),
            pltpu.VMEM(angle.shape, angle.dtype),
            pltpu.VMEM((high // LANES, 8, LANES), jnp.float32),
            pltpu.VMEM((high // LANES, 8, LANES), jnp.float32),
            pltpu.VMEM((rows, tile), jnp.float32),
            pltpu.VMEM((rows, tile), jnp.float32),
            pltpu.VMEM((high // LANES, rows // 8, LANES), jnp.bfloat16),
            pltpu.SemaphoreType.DMA((high // tile,)),
            pltpu.SemaphoreType.DMA((3,)),
            pltpu.SemaphoreType.DMA((high // LANES,)),
        ],
        compiler_params=pltpu.CompilerParams(vmem_limit_bytes=24 * MIB),
        cost_estimate=pl.CostEstimate(
            flops=2 * rows * low * high, bytes_accessed=2 * low * high, transcendentals=0
        ),
        name="lift",
    )(*(pltpu.with_memory_space_constraint(x, pltpu.HBM) for x in (octant, leaf, interp, angle)))


def translate_kernel(linked, count, *refs):
    tables = refs[:count]
    received, factors, interp_far, angle_far = refs[count : count + 4]
    out, kept, cosines, sines, source, angle, ready = refs[count + 4 :]
    kept_copy = pltpu.make_async_copy(interp_far, kept, ready.at[0])
    angle_copy = pltpu.make_async_copy(angle_far, angle, ready.at[1])
    angle_copy.start()
    kept_copy.start()
    source[...] = received[...].astype(jnp.float32).reshape(source.shape)
    half = received.shape[1] // 2
    owned = tables[0].shape[0]
    side = lax.axis_index("box")
    for shift, table in enumerate(tables):
        base = lax.rem(side + shift, count) * owned

        def target(p, carry, table=table, base=base):
            real = imag = None
            for k in range(linked):
                code = table[p, k]
                row = pl.multiple_of(code & 0xFFFF, 2 * half)
                pair = code >> 16
                re = source[pl.ds(row, half), :]
                im = source[pl.ds(row + half, half), :]
                f_re = factors[pl.ds(pair, 1), :]
                f_im = factors[pl.ds(pair + 1, 1), :]
                a = f_re * re - f_im * im
                b = f_re * im + f_im * re
                real = a if real is None else real + a
                imag = b if imag is None else imag + b
            out[base + p] = jnp.concatenate([real, imag], 0).astype(out.dtype)
            return carry

        lax.fori_loop(0, owned, target, 0)
    angle_copy.wait()
    phases(angle, cosines, sines)
    kept_copy.wait()


def translate(tables, received, factors, interp, angle):
    parents, rows, width = received.shape
    linked = tables[0].shape[1]
    count = len(tables)
    high = interp.shape[1]
    smem = pl.BlockSpec(memory_space=pltpu.SMEM)
    vmem = pl.BlockSpec(memory_space=pltpu.VMEM)
    far = pl.BlockSpec(memory_space=pltpu.HBM)
    phase = pltpu.VMEM((high // LANES, 8, LANES), jnp.float32)
    return pl.pallas_call(
        functools.partial(translate_kernel, linked, count),
        out_shape=(
            pltpu.VMEM(received.shape, jnp.bfloat16),
            pltpu.VMEM(interp.shape, interp.dtype),
            phase,
            phase,
        ),
        in_specs=[smem] * count + [vmem, vmem, far, far],
        out_specs=(vmem,) * 4,
        scratch_shapes=[
            pltpu.VMEM((parents * rows, width), jnp.float32),
            pltpu.VMEM(angle.shape, angle.dtype),
            pltpu.SemaphoreType.DMA((2,)),
        ],
        compiler_params=pltpu.CompilerParams(vmem_limit_bytes=24 * MIB),
        cost_estimate=pl.CostEstimate(
            flops=8 * parents * linked * rows * width, bytes_accessed=4 << 20, transcendentals=0
        ),
        name="translate",
    )(
        *tables,
        received,
        factors,
        *(pltpu.with_memory_space_constraint(x, pltpu.HBM) for x in (interp, angle)),
    )


def descend_kernel(
    place, scale, tile, octant, incoming, kept, cosines, sines, out, even, odd, total
):
    low, high = kept.shape
    count = high // tile
    boxes = even.shape[0] // PAIR

    def shift(i, shifted):
        for lane in range(0, tile, LANES):
            block = i * (tile // LANES) + lane // LANES
            received = incoming[place(block)].astype(jnp.float32)
            for child in range(boxes):
                which = octant[child]
                cos = cosines[block, pl.ds(which, 1), :]
                sin = sines[block, pl.ds(which, 1), :]
                row = PAIR * (child // 8)
                in_re = received[row : row + EXCITE]
                in_im = received[row + EXCITE : row + PAIR]
                re = in_re * cos + in_im * sin
                im = in_im * cos - in_re * sin
                both = jnp.concatenate([re, im], 0).astype(jnp.bfloat16)
                shifted[PAIR * child : PAIR * (child + 1), lane : lane + LANES] = both

    def drop(i, shifted):
        total[...] += lax.dot_general(
            kept[:, chunk_of(i, tile)],
            shifted[...],
            (((1,), (1,)), ((), ())),
            preferred_element_type=jnp.float32,
        )

    def two(j, carry):
        drop(2 * j, even)
        shift(2 * j + 1, odd)
        drop(2 * j + 1, odd)
        shift(jnp.minimum(2 * j + 2, count - 1), even)
        return carry

    total[...] = jnp.zeros_like(total)
    shift(0, even)
    lax.fori_loop(0, count // 2, two, 0)
    out[...] = (total[...].T * scale).astype(out.dtype)


def descend(incoming, octant, kept, cosines, sines, place):
    low, high = kept.shape
    rows = incoming.shape[1] * 8
    tile = 512
    near = pl.BlockSpec(memory_space=pltpu.VMEM)
    return pl.pallas_call(
        functools.partial(descend_kernel, place, low / high, tile),
        out_shape=jax.ShapeDtypeStruct((rows, low), jnp.bfloat16),
        in_specs=[pl.BlockSpec(memory_space=pltpu.SMEM), near, near, near, near],
        out_specs=near,
        scratch_shapes=[
            pltpu.VMEM((rows, tile), jnp.bfloat16),
            pltpu.VMEM((rows, tile), jnp.bfloat16),
            pltpu.VMEM((low, rows), jnp.float32),
        ],
        compiler_params=pltpu.CompilerParams(vmem_limit_bytes=24 * MIB),
        cost_estimate=pl.CostEstimate(
            flops=2 * rows * low * high, bytes_accessed=2 * low * high, transcendentals=0
        ),
        name="descend",
    )(octant, incoming, kept, cosines, sines)


def local(leaf_patterns, octant, interp, shift_angle, partners, types, translators):
    boxes, pairs, excite, low = leaf_patterns.shape
    high = interp.shape[1]
    sides = lax.axis_size("box")
    groups = lax.axis_size("dir")
    devices = sides * groups
    axes = ("box", "dir")
    width = high // devices
    parents = boxes // 8
    rows = parents * PAIR
    direct = width == LANES

    def place(t):
        return lax.rem(t, sides) * groups + lax.div(t, sides) if direct else t

    outgoing = lift(leaf_patterns.reshape(-1, low), octant, interp, shift_angle, place)
    if not direct:
        outgoing = outgoing.transpose(1, 0, 2).reshape(rows, groups, sides, width)
        outgoing = outgoing.transpose(2, 1, 0, 3).reshape(devices, rows, width)
    received = lax.all_to_all(outgoing, axes, split_axis=0, concat_axis=0, tiled=True)
    received = received.reshape(devices * parents, PAIR, width)

    code = partners * PAIR | (types * 2 << 16)
    tables = [code] + [
        lax.ppermute(code, "box", [((s + shift) % sides, s) for s in range(sides)])
        for shift in range(1, sides)
    ]
    side = lax.axis_index("box")
    factors = lax.dynamic_slice_in_dim(translators, side * width, width, axis=2)
    incoming, kept, cosines, sines = translate(
        tables, received, factors.reshape(-1, width), interp, shift_angle
    )

    incoming = incoming.reshape(devices, rows, width)
    returned = lax.all_to_all(incoming, axes, split_axis=0, concat_axis=0, tiled=True)
    if not direct:
        returned = returned.reshape(sides, groups, rows, width).transpose(2, 1, 0, 3)
        returned = returned.reshape(rows, high // LANES, LANES).transpose(1, 0, 2)
    down = descend(returned, octant, kept, cosines, sines, place)
    return down.reshape(boxes, pairs, excite, low)


def solution(mesh):
    placed = (
        P(("box", "dir"), None, None, None),
        P(("box", "dir")),
        P(),
        P(),
        P("box", None),
        P("box", None),
        P(None, None, "dir"),
    )
    return jax.shard_map(
        local,
        mesh=mesh,
        in_specs=placed,
        out_specs=P(("box", "dir"), None, None, None),
        check_vma=False,
    )
```

```python
import functools

import jax
import jax.numpy as jnp
from jax import lax
from jax.experimental import pallas as pl
from jax.experimental.pallas import tpu as pltpu
from jax.sharding import PartitionSpec as P

LANES = 128
EXCITE = 8
PAIR = 2 * EXCITE
MIB = 1 << 20
AHEAD = 2
TILE3 = 1024


def sincos(x):
    turns = jnp.floor(x * 0.6366197723675814 + 0.5)
    r = x - turns * 1.5703125
    r = r - turns * 4.837512969970703e-4
    r = r - turns * 7.549789948768648e-8
    z = r * r
    s = ((-1.9515295891e-4 * z + 8.3321608736e-3) * z - 1.6666654611e-1) * z * r + r
    c = ((2.443315711809948e-5 * z - 1.388731625493765e-3) * z + 4.166664568298827e-2) * z * z
    c = c - 0.5 * z + 1.0
    quadrant = turns.astype(jnp.int32)
    odd = (quadrant & 1) == 1
    sine = jnp.where(odd, c, s)
    cosine = jnp.where(odd, s, c)
    sine = jnp.where((quadrant & 2) == 2, -sine, sine)
    cosine = jnp.where(((quadrant + 1) & 2) == 2, -cosine, cosine)
    return cosine, sine


def phases(angle, cosines, sines):
    def block(b, carry):
        lanes = pl.ds(pl.multiple_of(b * LANES, LANES), LANES)
        cosines[b], sines[b] = sincos(angle[:, lanes])
        return carry

    lax.fori_loop(0, cosines.shape[0], block, 0, unroll=4)


def chunk_of(i, tile):
    return pl.ds(pl.multiple_of(i * tile, tile), tile)


def column_copy(far, near, arrived, tile, i):
    columns = chunk_of(i, tile)
    return pltpu.make_async_copy(far.at[:, columns], near.at[:, columns], arrived.at[i])


def lift_kernel(
    place, tile, octant_far, leaf_far, interp_far, angle_far, out_far, cosines_far, sines_far,
    octant, leaf, interp, angle, cosines, sines, up_even, up_odd, out, arrived, ready, sent,
):
    low, high = interp.shape
    count = high // tile
    boxes = leaf.shape[0] // PAIR
    angle_copy = pltpu.make_async_copy(angle_far, angle, ready.at[0])
    leaf_copy = pltpu.make_async_copy(leaf_far, leaf, ready.at[1])
    octant_copy = pltpu.make_async_copy(octant_far, octant, ready.at[2])
    angle_copy.start()
    octant_copy.start()
    leaf_copy.start()
    ahead = min(AHEAD, count)
    for i in range(ahead):
        column_copy(interp_far, interp, arrived, tile, i).start()
    angle_copy.wait()
    phases(angle, cosines, sines)
    cosines_copy = pltpu.make_async_copy(cosines, cosines_far, ready.at[3])
    sines_copy = pltpu.make_async_copy(sines, sines_far, ready.at[4])
    cosines_copy.start()
    sines_copy.start()
    octant_copy.wait()
    leaf_copy.wait()

    def send(i, first, last):
        for part in range(tile // LANES):
            block = place(i * (tile // LANES) + part)
            copy = pltpu.make_async_copy(out.at[block], out_far.at[block], sent.at[block])
            copy.start() if first else None
            copy.wait() if last else None

    def rise(i, up):
        column_copy(interp_far, interp, arrived, tile, i).wait()

        @pl.when(i + ahead < count)
        def _():
            column_copy(interp_far, interp, arrived, tile, i + ahead).start()

        up[...] = jnp.dot(
            leaf[...], interp[:, chunk_of(i, tile)], preferred_element_type=jnp.float32
        )

    def combine(i, up):
        for lane in range(0, tile, LANES):
            block = i * (tile // LANES) + lane // LANES
            for parent in range(boxes // 8):
                real = imag = None
                for child in range(8 * parent, 8 * parent + 8):
                    which = octant[child]
                    cos = cosines[block, pl.ds(which, 1), :]
                    sin = sines[block, pl.ds(which, 1), :]
                    row = PAIR * child
                    up_re = up[row : row + EXCITE, lane : lane + LANES]
                    up_im = up[row + EXCITE : row + PAIR, lane : lane + LANES]
                    re = up_re * cos - up_im * sin
                    im = up_re * sin + up_im * cos
                    real = re if real is None else real + re
                    imag = im if imag is None else imag + im
                both = jnp.concatenate([real, imag], 0).astype(jnp.bfloat16)
                out[place(block), PAIR * parent : PAIR * (parent + 1), :] = both

    def two(j, carry):
        @pl.when(j > 0)
        def _():
            send(2 * j - 2, True, False)

        rise(2 * j, up_even)
        combine(jnp.maximum(2 * j - 1, 0), up_odd)
        rise(2 * j + 1, up_odd)
        combine(2 * j, up_even)
        return carry

    lax.fori_loop(0, count // 2, two, 0)
    combine(count - 1, up_odd)
    for i in range(count):
        if i % 2 or i + 2 >= count:
            send(i, True, False)
    for i in range(count):
        send(i, False, True)
    cosines_copy.wait()
    sines_copy.wait()


def lift(leaf, octant, interp, angle, place):
    rows, low = leaf.shape
    high = interp.shape[1]
    tile = 1024
    far = pl.BlockSpec(memory_space=pltpu.HBM)
    phase = pltpu.HBM((high // LANES, 8, LANES), jnp.float32)
    return pl.pallas_call(
        functools.partial(lift_kernel, place, tile),
        out_shape=(
            jax.ShapeDtypeStruct((high // LANES, rows // 8, LANES), jnp.bfloat16),
            phase,
            phase,
        ),
        in_specs=[far, far, far, far],
        out_specs=(far, far, far),
        scratch_shapes=[
            pltpu.SMEM(octant.shape, octant.dtype),
            pltpu.VMEM(leaf.shape, leaf.dtype),
            pltpu.VMEM(interp.shape, interp.dtype),
            pltpu.VMEM(angle.shape, angle.dtype),
            pltpu.VMEM((high // LANES, 8, LANES), jnp.float32),
            pltpu.VMEM((high // LANES, 8, LANES), jnp.float32),
            pltpu.VMEM((rows, tile), jnp.float32),
            pltpu.VMEM((rows, tile), jnp.float32),
            pltpu.VMEM((high // LANES, rows // 8, LANES), jnp.bfloat16),
            pltpu.SemaphoreType.DMA((high // tile,)),
            pltpu.SemaphoreType.DMA((5,)),
            pltpu.SemaphoreType.DMA((high // LANES,)),
        ],
        compiler_params=pltpu.CompilerParams(vmem_limit_bytes=24 * MIB),
        cost_estimate=pl.CostEstimate(
            flops=2 * rows * low * high, bytes_accessed=2 * low * high, transcendentals=0
        ),
        name="lift",
    )(*(pltpu.with_memory_space_constraint(x, pltpu.HBM) for x in (octant, leaf, interp, angle)))


def grid_slot(index, bits):
    slot = 0
    for bit in range(bits):
        slot = slot + ((index >> bit) & 1) * ((49, 7, 1)[bit % 3] << (bit // 3))
    return slot


def translate_grid_kernel(linked, bits, count, *refs):
    tables = refs[:count]
    received, factors, out, source = refs[count:]
    lead = 3 * (49 + 7 + 1) * EXCITE
    last = grid_slot(received.shape[0] - 1, bits) * EXCITE
    imag_at = lead + last + EXCITE
    span = source.shape[0] - last
    for parent in range(received.shape[0]):
        both = received[parent].astype(jnp.float32)
        row = lead + grid_slot(parent, bits) * EXCITE
        source[row : row + EXCITE, :] = both[:EXCITE]
        source[imag_at + row : imag_at + row + EXCITE, :] = both[EXCITE:]
    owned = tables[0].shape[0]
    side = lax.axis_index("box")
    for shift, table in enumerate(tables):
        base = lax.rem(side + shift, count) * owned

        def target(p, carry, table=table, base=base):
            real = imag = None
            start = pl.multiple_of(table[p, linked], EXCITE)
            view = source.at[pl.ds(start, span)]
            for k in range(linked):
                row = pl.multiple_of(table[p, k], EXCITE)
                re = view[pl.ds(row, EXCITE), :]
                im = view[pl.ds(row + imag_at, EXCITE), :]
                f_re = factors[pl.ds(row, 1), :]
                f_im = factors[pl.ds(row + 1, 1), :]
                a = f_re * re - f_im * im
                b = f_re * im + f_im * re
                real = a if real is None else real + a
                imag = b if imag is None else imag + b
            out[base + p] = jnp.concatenate([real, imag], 0).astype(out.dtype)
            return carry

        lax.fori_loop(0, owned, target, 0, unroll=2)


def translate_kernel(linked, count, *refs):
    tables = refs[:count]
    received, factors, out, source = refs[count:]
    source[...] = received[...].astype(jnp.float32).reshape(source.shape)
    owned = tables[0].shape[0]
    side = lax.axis_index("box")
    for shift, table in enumerate(tables):
        base = lax.rem(side + shift, count) * owned

        def target(p, carry, table=table, base=base):
            real = imag = None
            for k in range(linked):
                code = table[p, k]
                row = pl.multiple_of(code & 0xFFFF, PAIR)
                pair = pl.multiple_of(code >> 16, EXCITE)
                re = source[pl.ds(row, EXCITE), :]
                im = source[pl.ds(row + EXCITE, EXCITE), :]
                f_re = factors[pl.ds(pair, 1), :]
                f_im = factors[pl.ds(pair + 1, 1), :]
                a = f_re * re - f_im * im
                b = f_re * im + f_im * re
                real = a if real is None else real + a
                imag = b if imag is None else imag + b
            out[base + p] = jnp.concatenate([real, imag], 0).astype(out.dtype)
            return carry

        lax.fori_loop(0, owned, target, 0)


def translate(tables, received, factors, linked, bits):
    parents, rows, width = received.shape
    count = len(tables)
    smem = pl.BlockSpec(memory_space=pltpu.SMEM)
    vmem = pl.BlockSpec(memory_space=pltpu.VMEM)
    if bits is None:
        kernel = functools.partial(translate_kernel, linked, count)
        source = parents * rows
    else:
        kernel = functools.partial(translate_grid_kernel, linked, bits, count)
        source = (2 * grid_slot(parents - 1, bits) + 2 + 9 * (49 + 7 + 1)) * EXCITE
    return pl.pallas_call(
        kernel,
        out_shape=jax.ShapeDtypeStruct(received.shape, jnp.bfloat16),
        in_specs=[smem] * count + [vmem, vmem],
        out_specs=vmem,
        scratch_shapes=[pltpu.VMEM((source, width), jnp.float32)],
        compiler_params=pltpu.CompilerParams(vmem_limit_bytes=12 * MIB),
        cost_estimate=pl.CostEstimate(flops=4 << 30, bytes_accessed=4 << 20, transcendentals=0),
        name="translate",
    )(*tables, received, factors)


def descend_kernel(
    place, scale, tile, octant_far, incoming, interp, cosines, sines, out_far,
    octant, even, odd, total, out, sent, ready,
):
    low, high = interp.shape
    count = high // tile
    boxes = even.shape[0] // PAIR
    octant_copy = pltpu.make_async_copy(octant_far, octant, ready)
    octant_copy.start()
    octant_copy.wait()

    def shift(i, shifted):
        for lane in range(0, tile, LANES):
            block = i * (tile // LANES) + lane // LANES
            received = incoming[place(block)].astype(jnp.float32)
            for child in range(boxes):
                which = octant[child]
                cos = cosines[block, pl.ds(which, 1), :]
                sin = sines[block, pl.ds(which, 1), :]
                row = PAIR * (child // 8)
                in_re = received[row : row + EXCITE]
                in_im = received[row + EXCITE : row + PAIR]
                re = in_re * cos + in_im * sin
                im = in_im * cos - in_re * sin
                both = jnp.concatenate([re, im], 0).astype(jnp.bfloat16)
                shifted[PAIR * child : PAIR * (child + 1), lane : lane + LANES] = both

    halves = (even, odd)
    shift(0, even)
    for i in range(count):
        part = lax.dot_general(
            interp[:, i * tile : (i + 1) * tile],
            halves[i % 2][...],
            (((1,), (1,)), ((), ())),
            preferred_element_type=jnp.float32,
        )
        total[...] = part if i == 0 else total[...] + part
        if i + 1 < count:
            shift(i + 1, halves[(i + 1) % 2])
    step = low // sent.shape[0]
    copies = []
    for i in range(sent.shape[0]):
        columns = pl.ds(i * step, step)
        out[:, columns] = (total[columns, :].T * scale).astype(out.dtype)
        copies.append(pltpu.make_async_copy(out.at[:, columns], out_far.at[:, columns], sent.at[i]))
        copies[-1].start()
    for copy in copies:
        copy.wait()


def descend(incoming, octant, interp, cosines, sines, place):
    low, high = interp.shape
    rows = incoming.shape[1] * 8
    tile = TILE3
    near = pl.BlockSpec(memory_space=pltpu.VMEM)
    far = pl.BlockSpec(memory_space=pltpu.HBM)
    octant = pltpu.with_memory_space_constraint(octant, pltpu.HBM)
    return pl.pallas_call(
        functools.partial(descend_kernel, place, low / high, tile),
        out_shape=jax.ShapeDtypeStruct((rows, low), jnp.bfloat16),
        in_specs=[far, near, near, near, near],
        out_specs=far,
        scratch_shapes=[
            pltpu.SMEM(octant.shape, octant.dtype),
            pltpu.VMEM((rows, tile), jnp.bfloat16),
            pltpu.VMEM((rows, tile), jnp.bfloat16),
            pltpu.VMEM((low, rows), jnp.float32),
            pltpu.VMEM((rows, low), jnp.bfloat16),
            pltpu.SemaphoreType.DMA((4,)),
            pltpu.SemaphoreType.DMA(()),
        ],
        compiler_params=pltpu.CompilerParams(vmem_limit_bytes=12 * MIB),
        cost_estimate=pl.CostEstimate(
            flops=2 * rows * low * high, bytes_accessed=2 * low * high, transcendentals=0
        ),
        name="descend",
    )(octant, incoming, interp, cosines, sines)


def local(leaf_patterns, octant, interp, shift_angle, partners, types, translators):
    boxes, pairs, excite, low = leaf_patterns.shape
    high = interp.shape[1]
    sides = lax.axis_size("box")
    groups = lax.axis_size("dir")
    devices = sides * groups
    axes = ("box", "dir")
    width = high // devices
    parents = boxes // 8
    rows = parents * PAIR
    direct = width == LANES

    def place(t):
        return lax.rem(t, sides) * groups + lax.div(t, sides) if direct else t

    outgoing, cosines, sines = lift(leaf_patterns.reshape(-1, low), octant, interp, shift_angle, place)
    if not direct:
        outgoing = outgoing.transpose(1, 0, 2).reshape(rows, groups, sides, width)
        outgoing = outgoing.transpose(2, 1, 0, 3).reshape(devices, rows, width)
    received = lax.all_to_all(outgoing, axes, split_axis=0, concat_axis=0, tiled=True)
    received = received.reshape(devices * parents, PAIR, width)

    side = lax.axis_index("box")
    owned, linked = types.shape
    bits = (devices * parents - 1).bit_length()
    extent = 1 << (bits + 2) // 3
    if extent <= 7:
        own = side * owned + jnp.arange(owned, dtype=jnp.int32)
        start = grid_slot(own, bits)
        code = jnp.concatenate([types, start[:, None]], 1) * EXCITE
    else:
        bits = None
        code = partners * PAIR | (types * EXCITE << 16)
    tables = [code] + [
        lax.ppermute(code, "box", [((s + shift) % sides, s) for s in range(sides)])
        for shift in range(1, sides)
    ]
    factors = lax.dynamic_slice_in_dim(translators, side * width, width, axis=2)
    factors = jnp.pad(factors, ((0, 0), (0, EXCITE - 2), (0, 0))).reshape(-1, width)
    incoming = translate(tables, received, factors, linked, bits)

    incoming = incoming.reshape(devices, rows, width)
    returned = lax.all_to_all(incoming, axes, split_axis=0, concat_axis=0, tiled=True)
    if not direct:
        returned = returned.reshape(sides, groups, rows, width).transpose(2, 1, 0, 3)
        returned = returned.reshape(rows, high // LANES, LANES).transpose(1, 0, 2)
    down = descend(returned, octant, interp, cosines, sines, place)
    return down.reshape(boxes, pairs, excite, low)


def solution(mesh):
    placed = (
        P(("box", "dir"), None, None, None),
        P(("box", "dir")),
        P(),
        P(),
        P("box", None),
        P("box", None),
        P(None, None, "dir"),
    )
    return jax.shard_map(
        local,
        mesh=mesh,
        in_specs=placed,
        out_specs=P(("box", "dir"), None, None, None),
        check_vma=False,
    )
```

```python
import functools

import jax
import jax.numpy as jnp
from jax import lax
from jax.experimental import pallas as pl
from jax.experimental.pallas import tpu as pltpu
from jax.sharding import PartitionSpec as P

LANES = 128
EXCITE = 8
PAIR = 2 * EXCITE
MIB = 1 << 20
AHEAD = 2
TILE3 = 512


def sincos(x):
    turns = jnp.floor(x * 0.6366197723675814 + 0.5)
    r = x - turns * 1.5703125
    r = r - turns * 4.837512969970703e-4
    r = r - turns * 7.549789948768648e-8
    z = r * r
    s = ((-1.9515295891e-4 * z + 8.3321608736e-3) * z - 1.6666654611e-1) * z * r + r
    c = ((2.443315711809948e-5 * z - 1.388731625493765e-3) * z + 4.166664568298827e-2) * z * z
    c = c - 0.5 * z + 1.0
    quadrant = turns.astype(jnp.int32)
    odd = (quadrant & 1) == 1
    sine = jnp.where(odd, c, s)
    cosine = jnp.where(odd, s, c)
    sine = jnp.where((quadrant & 2) == 2, -sine, sine)
    cosine = jnp.where(((quadrant + 1) & 2) == 2, -cosine, cosine)
    return cosine, sine


def phases(angle, cosines, sines):
    def block(b, carry):
        lanes = pl.ds(pl.multiple_of(b * LANES, LANES), LANES)
        cosines[b], sines[b] = sincos(angle[:, lanes])
        return carry

    lax.fori_loop(0, cosines.shape[0], block, 0, unroll=4)


def chunk_of(i, tile):
    return pl.ds(pl.multiple_of(i * tile, tile), tile)


def column_copy(far, near, arrived, tile, i):
    columns = chunk_of(i, tile)
    return pltpu.make_async_copy(far.at[:, columns], near.at[:, columns], arrived.at[i])


def lift_kernel(
    place, tile, octant_far, leaf_far, interp_far, angle_far, out_far, cosines_far, sines_far,
    octant, leaf, interp, angle, cosines, sines, up_even, up_odd, out, arrived, ready, sent,
):
    low, high = interp.shape
    count = high // tile
    boxes = leaf.shape[0] // PAIR
    angle_copy = pltpu.make_async_copy(angle_far, angle, ready.at[0])
    leaf_copy = pltpu.make_async_copy(leaf_far, leaf, ready.at[1])
    octant_copy = pltpu.make_async_copy(octant_far, octant, ready.at[2])
    angle_copy.start()
    octant_copy.start()
    leaf_copy.start()
    ahead = min(AHEAD, count)
    for i in range(ahead):
        column_copy(interp_far, interp, arrived, tile, i).start()
    angle_copy.wait()
    phases(angle, cosines, sines)
    cosines_copy = pltpu.make_async_copy(cosines, cosines_far, ready.at[3])
    sines_copy = pltpu.make_async_copy(sines, sines_far, ready.at[4])
    cosines_copy.start()
    sines_copy.start()
    octant_copy.wait()
    leaf_copy.wait()

    def send(i, first, last):
        for part in range(tile // LANES):
            block = place(i * (tile // LANES) + part)
            copy = pltpu.make_async_copy(out.at[block], out_far.at[block], sent.at[block])
            copy.start() if first else None
            copy.wait() if last else None

    def rise(i, up):
        column_copy(interp_far, interp, arrived, tile, i).wait()

        @pl.when(i + ahead < count)
        def _():
            column_copy(interp_far, interp, arrived, tile, i + ahead).start()

        up[...] = jnp.dot(
            leaf[...], interp[:, chunk_of(i, tile)], preferred_element_type=jnp.float32
        )

    def combine(i, up):
        for lane in range(0, tile, LANES):
            block = i * (tile // LANES) + lane // LANES
            for parent in range(boxes // 8):
                real = imag = None
                for child in range(8 * parent, 8 * parent + 8):
                    which = octant[child]
                    cos = cosines[block, pl.ds(which, 1), :]
                    sin = sines[block, pl.ds(which, 1), :]
                    row = PAIR * child
                    up_re = up[row : row + EXCITE, lane : lane + LANES]
                    up_im = up[row + EXCITE : row + PAIR, lane : lane + LANES]
                    re = up_re * cos - up_im * sin
                    im = up_re * sin + up_im * cos
                    real = re if real is None else real + re
                    imag = im if imag is None else imag + im
                both = jnp.concatenate([real, imag], 0).astype(jnp.bfloat16)
                out[place(block), PAIR * parent : PAIR * (parent + 1), :] = both

    def two(j, carry):
        @pl.when(j > 0)
        def _():
            send(2 * j - 2, True, False)

        rise(2 * j, up_even)
        combine(jnp.maximum(2 * j - 1, 0), up_odd)
        rise(2 * j + 1, up_odd)
        combine(2 * j, up_even)
        return carry

    lax.fori_loop(0, count // 2, two, 0)
    combine(count - 1, up_odd)
    for i in range(count):
        if i % 2 or i + 2 >= count:
            send(i, True, False)
    for i in range(count):
        send(i, False, True)
    cosines_copy.wait()
    sines_copy.wait()


def lift(leaf, octant, interp, angle, place):
    rows, low = leaf.shape
    high = interp.shape[1]
    tile = 1024
    far = pl.BlockSpec(memory_space=pltpu.HBM)
    phase = pltpu.HBM((high // LANES, 8, LANES), jnp.float32)
    return pl.pallas_call(
        functools.partial(lift_kernel, place, tile),
        out_shape=(
            jax.ShapeDtypeStruct((high // LANES, rows // 8, LANES), jnp.bfloat16),
            phase,
            phase,
        ),
        in_specs=[far, far, far, far],
        out_specs=(far, far, far),
        scratch_shapes=[
            pltpu.SMEM(octant.shape, octant.dtype),
            pltpu.VMEM(leaf.shape, leaf.dtype),
            pltpu.VMEM(interp.shape, interp.dtype),
            pltpu.VMEM(angle.shape, angle.dtype),
            pltpu.VMEM((high // LANES, 8, LANES), jnp.float32),
            pltpu.VMEM((high // LANES, 8, LANES), jnp.float32),
            pltpu.VMEM((rows, tile), jnp.float32),
            pltpu.VMEM((rows, tile), jnp.float32),
            pltpu.VMEM((high // LANES, rows // 8, LANES), jnp.bfloat16),
            pltpu.SemaphoreType.DMA((high // tile,)),
            pltpu.SemaphoreType.DMA((5,)),
            pltpu.SemaphoreType.DMA((high // LANES,)),
        ],
        compiler_params=pltpu.CompilerParams(vmem_limit_bytes=24 * MIB),
        cost_estimate=pl.CostEstimate(
            flops=2 * rows * low * high, bytes_accessed=2 * low * high, transcendentals=0
        ),
        name="lift",
    )(*(pltpu.with_memory_space_constraint(x, pltpu.HBM) for x in (octant, leaf, interp, angle)))


def grid_slot(index, bits):
    slot = 0
    for bit in range(bits):
        slot = slot + ((index >> bit) & 1) * ((49, 7, 1)[bit % 3] << (bit // 3))
    return slot


def translate_grid_kernel(linked, bits, count, *refs):
    tables = refs[:count]
    received, factors, out, source = refs[count:]
    lead = 3 * (49 + 7 + 1) * EXCITE
    last = grid_slot(received.shape[0] - 1, bits) * EXCITE
    imag_at = lead + last + EXCITE
    span = source.shape[0] - last
    for parent in range(received.shape[0]):
        both = received[parent].astype(jnp.float32)
        row = lead + grid_slot(parent, bits) * EXCITE
        source[row : row + EXCITE, :] = both[:EXCITE]
        source[imag_at + row : imag_at + row + EXCITE, :] = both[EXCITE:]
    owned = tables[0].shape[0]
    side = lax.axis_index("box")
    for shift, table in enumerate(tables):
        base = lax.rem(side + shift, count) * owned

        def target(p, carry, table=table, base=base):
            real = imag = None
            start = pl.multiple_of(table[p, linked], EXCITE)
            view = source.at[pl.ds(start, span)]
            for k in range(linked):
                row = pl.multiple_of(table[p, k], EXCITE)
                re = view[pl.ds(row, EXCITE), :]
                im = view[pl.ds(row + imag_at, EXCITE), :]
                f_re = factors[pl.ds(row, 1), :]
                f_im = factors[pl.ds(row + 1, 1), :]
                a = f_re * re - f_im * im
                b = f_re * im + f_im * re
                real = a if real is None else real + a
                imag = b if imag is None else imag + b
            out[base + p] = jnp.concatenate([real, imag], 0).astype(out.dtype)
            return carry

        lax.fori_loop(0, owned, target, 0, unroll=4)


def translate_kernel(linked, count, *refs):
    tables = refs[:count]
    received, factors, out, source = refs[count:]
    source[...] = received[...].astype(jnp.float32).reshape(source.shape)
    owned = tables[0].shape[0]
    side = lax.axis_index("box")
    for shift, table in enumerate(tables):
        base = lax.rem(side + shift, count) * owned

        def target(p, carry, table=table, base=base):
            real = imag = None
            for k in range(linked):
                code = table[p, k]
                row = pl.multiple_of(code & 0xFFFF, PAIR)
                pair = pl.multiple_of(code >> 16, EXCITE)
                re = source[pl.ds(row, EXCITE), :]
                im = source[pl.ds(row + EXCITE, EXCITE), :]
                f_re = factors[pl.ds(pair, 1), :]
                f_im = factors[pl.ds(pair + 1, 1), :]
                a = f_re * re - f_im * im
                b = f_re * im + f_im * re
                real = a if real is None else real + a
                imag = b if imag is None else imag + b
            out[base + p] = jnp.concatenate([real, imag], 0).astype(out.dtype)
            return carry

        lax.fori_loop(0, owned, target, 0)


def translate(tables, received, factors, linked, bits):
    parents, rows, width = received.shape
    count = len(tables)
    smem = pl.BlockSpec(memory_space=pltpu.SMEM)
    vmem = pl.BlockSpec(memory_space=pltpu.VMEM)
    if bits is None:
        kernel = functools.partial(translate_kernel, linked, count)
        source = parents * rows
    else:
        kernel = functools.partial(translate_grid_kernel, linked, bits, count)
        source = (2 * grid_slot(parents - 1, bits) + 2 + 9 * (49 + 7 + 1)) * EXCITE
    return pl.pallas_call(
        kernel,
        out_shape=jax.ShapeDtypeStruct(received.shape, jnp.bfloat16),
        in_specs=[smem] * count + [vmem, vmem],
        out_specs=vmem,
        scratch_shapes=[pltpu.VMEM((source, width), jnp.float32)],
        compiler_params=pltpu.CompilerParams(vmem_limit_bytes=12 * MIB),
        cost_estimate=pl.CostEstimate(flops=4 << 30, bytes_accessed=4 << 20, transcendentals=0),
        name="translate",
    )(*tables, received, factors)


def descend_kernel(
    place, scale, tile, octant, incoming, interp, cosines, sines, out_far,
    even, odd, total, out, sent,
):
    low, high = interp.shape
    count = high // tile
    boxes = even.shape[0] // PAIR

    def shift(i, shifted):
        for lane in range(0, tile, LANES):
            block = i * (tile // LANES) + lane // LANES
            received = incoming[place(block)].astype(jnp.float32)
            for child in range(boxes):
                which = octant[child]
                cos = cosines[block, pl.ds(which, 1), :]
                sin = sines[block, pl.ds(which, 1), :]
                row = PAIR * (child // 8)
                in_re = received[row : row + EXCITE]
                in_im = received[row + EXCITE : row + PAIR]
                re = in_re * cos + in_im * sin
                im = in_im * cos - in_re * sin
                both = jnp.concatenate([re, im], 0).astype(jnp.bfloat16)
                shifted[PAIR * child : PAIR * (child + 1), lane : lane + LANES] = both

    halves = (even, odd)
    shift(0, even)
    for i in range(count):
        part = lax.dot_general(
            interp[:, i * tile : (i + 1) * tile],
            halves[i % 2][...],
            (((1,), (1,)), ((), ())),
            preferred_element_type=jnp.float32,
        )
        total[...] = part if i == 0 else total[...] + part
        if i + 1 < count:
            shift(i + 1, halves[(i + 1) % 2])
    step = low // sent.shape[0]
    copies = []
    for i in range(sent.shape[0]):
        columns = pl.ds(i * step, step)
        out[:, columns] = (total[columns, :].T * scale).astype(out.dtype)
        copies.append(pltpu.make_async_copy(out.at[:, columns], out_far.at[:, columns], sent.at[i]))
        copies[-1].start()
    for copy in copies:
        copy.wait()


def descend(incoming, octant, interp, cosines, sines, place):
    low, high = interp.shape
    rows = incoming.shape[1] * 8
    tile = TILE3
    near = pl.BlockSpec(memory_space=pltpu.VMEM)
    far = pl.BlockSpec(memory_space=pltpu.HBM)
    return pl.pallas_call(
        functools.partial(descend_kernel, place, low / high, tile),
        out_shape=jax.ShapeDtypeStruct((rows, low), jnp.bfloat16),
        in_specs=[pl.BlockSpec(memory_space=pltpu.SMEM), near, near, near, near],
        out_specs=far,
        scratch_shapes=[
            pltpu.VMEM((rows, tile), jnp.bfloat16),
            pltpu.VMEM((rows, tile), jnp.bfloat16),
            pltpu.VMEM((low, rows), jnp.float32),
            pltpu.VMEM((rows, low), jnp.bfloat16),
            pltpu.SemaphoreType.DMA((8,)),
        ],
        compiler_params=pltpu.CompilerParams(vmem_limit_bytes=12 * MIB),
        cost_estimate=pl.CostEstimate(
            flops=2 * rows * low * high, bytes_accessed=2 * low * high, transcendentals=0
        ),
        name="descend",
    )(octant, incoming, interp, cosines, sines)


def local(leaf_patterns, octant, interp, shift_angle, partners, types, translators):
    boxes, pairs, excite, low = leaf_patterns.shape
    high = interp.shape[1]
    sides = lax.axis_size("box")
    groups = lax.axis_size("dir")
    devices = sides * groups
    axes = ("box", "dir")
    width = high // devices
    parents = boxes // 8
    rows = parents * PAIR
    direct = width == LANES

    def place(t):
        return lax.rem(t, sides) * groups + lax.div(t, sides) if direct else t

    outgoing, cosines, sines = lift(leaf_patterns.reshape(-1, low), octant, interp, shift_angle, place)
    if not direct:
        outgoing = outgoing.transpose(1, 0, 2).reshape(rows, groups, sides, width)
        outgoing = outgoing.transpose(2, 1, 0, 3).reshape(devices, rows, width)
    received = lax.all_to_all(outgoing, axes, split_axis=0, concat_axis=0, tiled=True)
    received = received.reshape(devices * parents, PAIR, width)

    side = lax.axis_index("box")
    owned, linked = types.shape
    bits = (devices * parents - 1).bit_length()
    extent = 1 << (bits + 2) // 3
    if extent <= 7:
        own = side * owned + jnp.arange(owned, dtype=jnp.int32)
        start = grid_slot(own, bits)
        code = jnp.concatenate([types, start[:, None]], 1) * EXCITE
    else:
        bits = None
        code = partners * PAIR | (types * EXCITE << 16)
    tables = [code] + [
        lax.ppermute(code, "box", [((s + shift) % sides, s) for s in range(sides)])
        for shift in range(1, sides)
    ]
    factors = lax.dynamic_slice_in_dim(translators, side * width, width, axis=2)
    factors = jnp.pad(factors, ((0, 0), (0, EXCITE - 2), (0, 0))).reshape(-1, width)
    incoming = translate(tables, received, factors, linked, bits)

    incoming = incoming.reshape(devices, rows, width)
    returned = lax.all_to_all(incoming, axes, split_axis=0, concat_axis=0, tiled=True)
    if not direct:
        returned = returned.reshape(sides, groups, rows, width).transpose(2, 1, 0, 3)
        returned = returned.reshape(rows, high // LANES, LANES).transpose(1, 0, 2)
    down = descend(returned, octant, interp, cosines, sines, place)
    return down.reshape(boxes, pairs, excite, low)


def solution(mesh):
    placed = (
        P(("box", "dir"), None, None, None),
        P(("box", "dir")),
        P(),
        P(),
        P("box", None),
        P("box", None),
        P(None, None, "dir"),
    )
    return jax.shard_map(
        local,
        mesh=mesh,
        in_specs=placed,
        out_specs=P(("box", "dir"), None, None, None),
        check_vma=False,
    )
```

```python
import functools

import jax
import jax.numpy as jnp
from jax import lax
from jax.experimental import pallas as pl
from jax.experimental.pallas import tpu as pltpu
from jax.sharding import PartitionSpec as P

LANES = 128
EXCITE = 8
PAIR = 2 * EXCITE
MIB = 1 << 20
AHEAD = 2
TILE3 = 512


def sincos(x):
    turns = jnp.floor(x * 0.6366197723675814 + 0.5)
    r = x - turns * 1.5703125
    r = r - turns * 4.837512969970703e-4
    r = r - turns * 7.549789948768648e-8
    z = r * r
    s = ((-1.9515295891e-4 * z + 8.3321608736e-3) * z - 1.6666654611e-1) * z * r + r
    c = ((2.443315711809948e-5 * z - 1.388731625493765e-3) * z + 4.166664568298827e-2) * z * z
    c = c - 0.5 * z + 1.0
    quadrant = turns.astype(jnp.int32)
    odd = (quadrant & 1) == 1
    sine = jnp.where(odd, c, s)
    cosine = jnp.where(odd, s, c)
    sine = jnp.where((quadrant & 2) == 2, -sine, sine)
    cosine = jnp.where(((quadrant + 1) & 2) == 2, -cosine, cosine)
    return cosine, sine


def phases(angle, cosines, sines):
    def block(b, carry):
        lanes = pl.ds(pl.multiple_of(b * LANES, LANES), LANES)
        cosines[b], sines[b] = sincos(angle[:, lanes])
        return carry

    lax.fori_loop(0, cosines.shape[0], block, 0, unroll=4)


def chunk_of(i, tile):
    return pl.ds(pl.multiple_of(i * tile, tile), tile)


def column_copy(far, near, arrived, tile, i):
    columns = chunk_of(i, tile)
    return pltpu.make_async_copy(far.at[:, columns], near.at[:, columns], arrived.at[i])


def lift_kernel(
    place, tile, octant_far, leaf_far, interp_far, angle_far, out_far, cosines_far, sines_far,
    octant, leaf, interp, angle, cosines, sines, up_even, up_odd, out, arrived, ready, sent,
):
    low, high = interp.shape
    count = high // tile
    boxes = leaf.shape[0] // PAIR
    angle_copy = pltpu.make_async_copy(angle_far, angle, ready.at[0])
    leaf_copy = pltpu.make_async_copy(leaf_far, leaf, ready.at[1])
    octant_copy = pltpu.make_async_copy(octant_far, octant, ready.at[2])
    angle_copy.start()
    octant_copy.start()
    leaf_copy.start()
    ahead = min(AHEAD, count)
    for i in range(ahead):
        column_copy(interp_far, interp, arrived, tile, i).start(priority=min(i, 1))
    angle_copy.wait()
    phases(angle, cosines, sines)
    cosines_copy = pltpu.make_async_copy(cosines, cosines_far, ready.at[3])
    sines_copy = pltpu.make_async_copy(sines, sines_far, ready.at[4])
    cosines_copy.start()
    sines_copy.start()
    octant_copy.wait()
    leaf_copy.wait()

    def send(i, first, last):
        for part in range(tile // LANES):
            block = place(i * (tile // LANES) + part)
            copy = pltpu.make_async_copy(out.at[block], out_far.at[block], sent.at[block])
            copy.start() if first else None
            copy.wait() if last else None

    def rise(i, up):
        column_copy(interp_far, interp, arrived, tile, i).wait()

        @pl.when(i == 0)
        def _():
            for later in range(ahead, count):
                column_copy(interp_far, interp, arrived, tile, later).start()

        up[...] = jnp.dot(
            leaf[...], interp[:, chunk_of(i, tile)], preferred_element_type=jnp.float32
        )

    def combine(i, up):
        for lane in range(0, tile, LANES):
            block = i * (tile // LANES) + lane // LANES
            for parent in range(boxes // 8):
                real = imag = None
                for child in range(8 * parent, 8 * parent + 8):
                    which = octant[child]
                    cos = cosines[block, pl.ds(which, 1), :]
                    sin = sines[block, pl.ds(which, 1), :]
                    row = PAIR * child
                    up_re = up[row : row + EXCITE, lane : lane + LANES]
                    up_im = up[row + EXCITE : row + PAIR, lane : lane + LANES]
                    re = up_re * cos - up_im * sin
                    im = up_re * sin + up_im * cos
                    real = re if real is None else real + re
                    imag = im if imag is None else imag + im
                both = jnp.concatenate([real, imag], 0).astype(jnp.bfloat16)
                out[place(block), PAIR * parent : PAIR * (parent + 1), :] = both

    def two(j, carry):
        @pl.when(j > 0)
        def _():
            send(2 * j - 2, True, False)

        rise(2 * j, up_even)
        combine(jnp.maximum(2 * j - 1, 0), up_odd)
        rise(2 * j + 1, up_odd)
        combine(2 * j, up_even)
        return carry

    lax.fori_loop(0, count // 2, two, 0)
    combine(count - 1, up_odd)
    for i in range(count):
        if i % 2 or i + 2 >= count:
            send(i, True, False)
    for i in range(count):
        send(i, False, True)
    cosines_copy.wait()
    sines_copy.wait()


def lift(leaf, octant, interp, angle, place):
    rows, low = leaf.shape
    high = interp.shape[1]
    tile = 1024
    far = pl.BlockSpec(memory_space=pltpu.HBM)
    phase = pltpu.HBM((high // LANES, 8, LANES), jnp.float32)
    return pl.pallas_call(
        functools.partial(lift_kernel, place, tile),
        out_shape=(
            jax.ShapeDtypeStruct((high // LANES, rows // 8, LANES), jnp.bfloat16),
            phase,
            phase,
        ),
        in_specs=[far, far, far, far],
        out_specs=(far, far, far),
        scratch_shapes=[
            pltpu.SMEM(octant.shape, octant.dtype),
            pltpu.VMEM(leaf.shape, leaf.dtype),
            pltpu.VMEM(interp.shape, interp.dtype),
            pltpu.VMEM(angle.shape, angle.dtype),
            pltpu.VMEM((high // LANES, 8, LANES), jnp.float32),
            pltpu.VMEM((high // LANES, 8, LANES), jnp.float32),
            pltpu.VMEM((rows, tile), jnp.float32),
            pltpu.VMEM((rows, tile), jnp.float32),
            pltpu.VMEM((high // LANES, rows // 8, LANES), jnp.bfloat16),
            pltpu.SemaphoreType.DMA((high // tile,)),
            pltpu.SemaphoreType.DMA((5,)),
            pltpu.SemaphoreType.DMA((high // LANES,)),
        ],
        compiler_params=pltpu.CompilerParams(vmem_limit_bytes=24 * MIB),
        cost_estimate=pl.CostEstimate(
            flops=2 * rows * low * high, bytes_accessed=2 * low * high, transcendentals=0
        ),
        name="lift",
    )(*(pltpu.with_memory_space_constraint(x, pltpu.HBM) for x in (octant, leaf, interp, angle)))


def grid_slot(index, bits):
    slot = 0
    for bit in range(bits):
        slot = slot + ((index >> bit) & 1) * ((49, 7, 1)[bit % 3] << (bit // 3))
    return slot


def translate_grid_kernel(linked, bits, count, *refs):
    tables = refs[:count]
    received, factors, out, source = refs[count:]
    lead = 3 * (49 + 7 + 1) * EXCITE
    last = grid_slot(received.shape[0] - 1, bits) * EXCITE
    imag_at = lead + last + EXCITE
    span = source.shape[0] - last
    for parent in range(received.shape[0]):
        both = received[parent].astype(jnp.float32)
        row = lead + grid_slot(parent, bits) * EXCITE
        source[row : row + EXCITE, :] = both[:EXCITE]
        source[imag_at + row : imag_at + row + EXCITE, :] = both[EXCITE:]
    owned = tables[0].shape[0]
    side = lax.axis_index("box")
    for shift, table in enumerate(tables):
        base = lax.rem(side + shift, count) * owned

        def target(p, carry, table=table, base=base):
            real = imag = None
            start = pl.multiple_of(table[p, linked], EXCITE)
            view = source.at[pl.ds(start, span)]
            for k in range(linked):
                row = pl.multiple_of(table[p, k], EXCITE)
                re = view[pl.ds(row, EXCITE), :]
                im = view[pl.ds(row + imag_at, EXCITE), :]
                f_re = factors[pl.ds(row, 1), :]
                f_im = factors[pl.ds(row + 1, 1), :]
                a = f_re * re - f_im * im
                b = f_re * im + f_im * re
                real = a if real is None else real + a
                imag = b if imag is None else imag + b
            out[base + p] = jnp.concatenate([real, imag], 0).astype(out.dtype)
            return carry

        lax.fori_loop(0, owned, target, 0, unroll=4)


def translate_kernel(linked, count, *refs):
    tables = refs[:count]
    received, factors, out, source = refs[count:]
    source[...] = received[...].astype(jnp.float32).reshape(source.shape)
    owned = tables[0].shape[0]
    side = lax.axis_index("box")
    for shift, table in enumerate(tables):
        base = lax.rem(side + shift, count) * owned

        def target(p, carry, table=table, base=base):
            real = imag = None
            for k in range(linked):
                code = table[p, k]
                row = pl.multiple_of(code & 0xFFFF, PAIR)
                pair = pl.multiple_of(code >> 16, EXCITE)
                re = source[pl.ds(row, EXCITE), :]
                im = source[pl.ds(row + EXCITE, EXCITE), :]
                f_re = factors[pl.ds(pair, 1), :]
                f_im = factors[pl.ds(pair + 1, 1), :]
                a = f_re * re - f_im * im
                b = f_re * im + f_im * re
                real = a if real is None else real + a
                imag = b if imag is None else imag + b
            out[base + p] = jnp.concatenate([real, imag], 0).astype(out.dtype)
            return carry

        lax.fori_loop(0, owned, target, 0)


def translate(tables, received, factors, linked, bits):
    parents, rows, width = received.shape
    count = len(tables)
    smem = pl.BlockSpec(memory_space=pltpu.SMEM)
    vmem = pl.BlockSpec(memory_space=pltpu.VMEM)
    if bits is None:
        kernel = functools.partial(translate_kernel, linked, count)
        source = parents * rows
    else:
        kernel = functools.partial(translate_grid_kernel, linked, bits, count)
        source = (2 * grid_slot(parents - 1, bits) + 2 + 9 * (49 + 7 + 1)) * EXCITE
    return pl.pallas_call(
        kernel,
        out_shape=jax.ShapeDtypeStruct(received.shape, jnp.bfloat16),
        in_specs=[smem] * count + [vmem, vmem],
        out_specs=vmem,
        scratch_shapes=[pltpu.VMEM((source, width), jnp.float32)],
        compiler_params=pltpu.CompilerParams(vmem_limit_bytes=12 * MIB),
        cost_estimate=pl.CostEstimate(flops=4 << 30, bytes_accessed=4 << 20, transcendentals=0),
        name="translate",
    )(*tables, received, factors)


def descend_kernel(
    place, scale, tile, octant, incoming, interp, cosines, sines, out_far,
    even, odd, total, out, sent,
):
    low, high = interp.shape
    count = high // tile
    boxes = even.shape[0] // PAIR

    def shift(i, shifted):
        for lane in range(0, tile, LANES):
            block = i * (tile // LANES) + lane // LANES
            received = incoming[place(block)].astype(jnp.float32)
            for child in range(boxes):
                which = octant[child]
                cos = cosines[block, pl.ds(which, 1), :]
                sin = sines[block, pl.ds(which, 1), :]
                row = PAIR * (child // 8)
                in_re = received[row : row + EXCITE]
                in_im = received[row + EXCITE : row + PAIR]
                re = in_re * cos + in_im * sin
                im = in_im * cos - in_re * sin
                both = jnp.concatenate([re, im], 0).astype(jnp.bfloat16)
                shifted[PAIR * child : PAIR * (child + 1), lane : lane + LANES] = both

    halves = (even, odd)
    shift(0, even)
    for i in range(count):
        part = lax.dot_general(
            interp[:, i * tile : (i + 1) * tile],
            halves[i % 2][...],
            (((1,), (1,)), ((), ())),
            preferred_element_type=jnp.float32,
        )
        total[...] = part if i == 0 else total[...] + part
        if i + 1 < count:
            shift(i + 1, halves[(i + 1) % 2])
    step = low // sent.shape[0]
    copies = []
    for i in range(sent.shape[0]):
        columns = pl.ds(i * step, step)
        out[:, columns] = (total[columns, :].T * scale).astype(out.dtype)
        copies.append(pltpu.make_async_copy(out.at[:, columns], out_far.at[:, columns], sent.at[i]))
        copies[-1].start()
    for copy in copies:
        copy.wait()


def descend(incoming, octant, interp, cosines, sines, place):
    low, high = interp.shape
    rows = incoming.shape[1] * 8
    tile = TILE3
    near = pl.BlockSpec(memory_space=pltpu.VMEM)
    far = pl.BlockSpec(memory_space=pltpu.HBM)
    return pl.pallas_call(
        functools.partial(descend_kernel, place, low / high, tile),
        out_shape=jax.ShapeDtypeStruct((rows, low), jnp.bfloat16),
        in_specs=[pl.BlockSpec(memory_space=pltpu.SMEM), near, near, near, near],
        out_specs=far,
        scratch_shapes=[
            pltpu.VMEM((rows, tile), jnp.bfloat16),
            pltpu.VMEM((rows, tile), jnp.bfloat16),
            pltpu.VMEM((low, rows), jnp.float32),
            pltpu.VMEM((rows, low), jnp.bfloat16),
            pltpu.SemaphoreType.DMA((8,)),
        ],
        compiler_params=pltpu.CompilerParams(vmem_limit_bytes=12 * MIB),
        cost_estimate=pl.CostEstimate(
            flops=2 * rows * low * high, bytes_accessed=2 * low * high, transcendentals=0
        ),
        name="descend",
    )(octant, incoming, interp, cosines, sines)


def local(leaf_patterns, octant, interp, shift_angle, partners, types, translators):
    boxes, pairs, excite, low = leaf_patterns.shape
    high = interp.shape[1]
    sides = lax.axis_size("box")
    groups = lax.axis_size("dir")
    devices = sides * groups
    axes = ("box", "dir")
    width = high // devices
    parents = boxes // 8
    rows = parents * PAIR
    direct = width == LANES

    def place(t):
        return lax.rem(t, sides) * groups + lax.div(t, sides) if direct else t

    outgoing, cosines, sines = lift(leaf_patterns.reshape(-1, low), octant, interp, shift_angle, place)
    if not direct:
        outgoing = outgoing.transpose(1, 0, 2).reshape(rows, groups, sides, width)
        outgoing = outgoing.transpose(2, 1, 0, 3).reshape(devices, rows, width)
    received = lax.all_to_all(outgoing, axes, split_axis=0, concat_axis=0, tiled=True)
    received = received.reshape(devices * parents, PAIR, width)

    side = lax.axis_index("box")
    owned, linked = types.shape
    bits = (devices * parents - 1).bit_length()
    extent = 1 << (bits + 2) // 3
    if extent <= 7:
        own = side * owned + jnp.arange(owned, dtype=jnp.int32)
        start = grid_slot(own, bits)
        code = jnp.concatenate([types, start[:, None]], 1) * EXCITE
    else:
        bits = None
        code = partners * PAIR | (types * EXCITE << 16)
    tables = [code] + [
        lax.ppermute(code, "box", [((s + shift) % sides, s) for s in range(sides)])
        for shift in range(1, sides)
    ]
    factors = lax.dynamic_slice_in_dim(translators, side * width, width, axis=2)
    factors = jnp.pad(factors, ((0, 0), (0, EXCITE - 2), (0, 0))).reshape(-1, width)
    incoming = translate(tables, received, factors, linked, bits)

    incoming = incoming.reshape(devices, rows, width)
    returned = lax.all_to_all(incoming, axes, split_axis=0, concat_axis=0, tiled=True)
    if not direct:
        returned = returned.reshape(sides, groups, rows, width).transpose(2, 1, 0, 3)
        returned = returned.reshape(rows, high // LANES, LANES).transpose(1, 0, 2)
    down = descend(returned, octant, interp, cosines, sines, place)
    return down.reshape(boxes, pairs, excite, low)


def solution(mesh):
    placed = (
        P(("box", "dir"), None, None, None),
        P(("box", "dir")),
        P(),
        P(),
        P("box", None),
        P("box", None),
        P(None, None, "dir"),
    )
    return jax.shard_map(
        local,
        mesh=mesh,
        in_specs=placed,
        out_specs=P(("box", "dir"), None, None, None),
        check_vma=False,
    )
```
